32 devices in a mesh: seq: 8 (over z, y), grp: 4 (over x, core).
Axes of the slice: x: 2, y: 2, z: 4, core: 2. Of those that a mesh axis runs over, the one named last changes fastest.
Arguments:
- queries: bfloat16 [8192, 1024], P(('seq', 'grp')), may hold values from -5 to 5
- key_rows: bfloat16 [8192, 128], P(('seq', 'grp')), may hold values from -5 to 5
- value_rows: bfloat16 [8192, 128], P(('seq', 'grp')), may hold values from -6 to 6
- out_grad: bfloat16 [8192, 1024], P(('seq', 'grp')), may hold values from -6 to 6
- segment: int32 [8192], P(('seq', 'grp')), may hold values from 0 to 9, never falling along the last dimension, each value on 1 to 1536 neighbouring positions
Outputs:
- attended: bfloat16 [8192, 1024], P(('seq', 'grp'))
- query_grad: bfloat16 [8192, 1024], P(('seq', 'grp'))
- key_grad: float32 [8192, 128], P(('seq', 'grp'))
- value_grad: float32 [8192, 128], P(('seq', 'grp'))
The draws below stay inside these ranges and needn't reach their ends.
Inputs may be any that keep to these rules, and one draw needn't show every extreme that they name: `segment`: segment numbers start at 0 and never fall along the sequence; every document holds 1 to 1536 tokens, and one holds exactly 1536.
All inputs are finite; a program needn't handle non-finite values.
Results may differ from the reference program's by a relative error of at most 0.019.
Values may be sent and summed in bfloat16 or wider, within the bound.
A program may use at most 64 MiB of HBM per device.

```python
import math
import jax
import jax.numpy as jnp
import numpy as np
from jax import lax

HEADS = 8
HD = 128
TOK_DEV = 256
MAXDOC = 1536
TOKENS = 8192
SEGMENTS = 10


def pair_draw(key):
    base = jax.random.fold_in(key, 7)
    streams = jax.random.split(base, 2)
    query_draw = jnp.clip(jax.random.normal(streams[0], (TOKENS, HEADS * HD), jnp.float32), -5.0, 5.0)
    key_draw = jnp.clip(jax.random.normal(streams[1], (TOKENS, HD), jnp.float32), -5.0, 5.0)
    return (query_draw, key_draw)


def draw_queries(key, part):
    return pair_draw(key)[0].astype(jnp.bfloat16)


def draw_key_rows(key, part):
    return pair_draw(key)[1].astype(jnp.bfloat16)


def steps_of(own_key, shape, pieces, smallest, high):
    factor_of = 1.0
    for axis_at, parts in pieces:
        draws = jax.random.uniform(jax.random.fold_in(jax.random.fold_in(own_key, 6), axis_at), (parts,), jnp.float32, smallest / len(pieces), high / len(pieces))
        factor_of = factor_of * jnp.repeat(jnp.exp(draws), shape[axis_at] // parts).reshape((-1,) + (1,) * (len(shape) - 1 - axis_at))
    return factor_of


def length_profile(count, total, bound, slope):
    loads = [(1 << 20) // math.isqrt(standing ** slope) + 1 for standing in range(2, count + 1)]
    rest, counts = total - bound - (count - 1), [1] * (count - 1)
    while rest > 0:
        free = [i for i in range(count - 1) if counts[i] < bound]
        whole, budget = sum([loads[i] for i in free]), rest
        for i in free:
            addition = min(bound - counts[i], max(1, budget * loads[i] // whole), rest)
            counts[i] = counts[i] + addition
            rest = rest - addition
    return np.array([bound] + counts)


def ragged(own_key, count, total, limit, slope):
    if count == 2:
        one = jax.random.randint(own_key, (), max(1, total - limit), min(limit, total - 1) + 1)
        return jnp.stack([one, total - one])
    tallies = jnp.asarray(length_profile(count, total, limit, slope), jnp.int32)
    couples = (count - 1) // 2
    donor, sink = tallies[1:1 + 2 * couples:2], tallies[2:2 + 2 * couples:2]
    room = jnp.minimum(donor - 1, limit - sink)
    shifted = jax.random.randint(jax.random.fold_in(own_key, 1), (couples,), 0, 1 << 20) % (room + 1)
    tallies = tallies.at[1:1 + 2 * couples:2].set(donor - shifted).at[2:2 + 2 * couples:2].set(sink + shifted)
    return tallies[jax.random.permutation(jax.random.fold_in(own_key, 2), count)]


def normal_values(key, extent, scale, most, cuts=(), kind=jnp.bfloat16):
    result = scale * jax.random.normal(key, extent, jnp.float32)
    if cuts:
        result = result * steps_of(key, extent, cuts, -0.22, 0.18)
    return jnp.clip(result, -most, most).astype(kind)


def setup_inputs(seed: int = 0) -> dict:
    seeds = jax.random.split(jax.random.key(seed), 6)
    queries = draw_queries(jax.random.fold_in(seeds[5], 71), 0)
    key_rows = draw_key_rows(jax.random.fold_in(seeds[5], 71), 0)
    value_rows = normal_values(seeds[2], (TOKENS, HD), 1.0, 6.0, ((0, 32),))
    out_grad = normal_values(seeds[3], (TOKENS, HEADS * HD), 1.0, 6.0, ((0, 32),))
    segment = jnp.searchsorted(jnp.cumsum(ragged(seeds[4], SEGMENTS, TOKENS, MAXDOC, 1)), jnp.arange(TOKENS), side="right").astype(jnp.int32)
    return dict(queries=queries, key_rows=key_rows, value_rows=value_rows, out_grad=out_grad, segment=segment)


def reference(queries, key_rows, value_rows, out_grad, segment):
    score_scale = HD ** -0.5
    block_rows = 512 if TOKENS % 512 == 0 else TOK_DEV
    block_count = TOKENS // block_rows
    window = MAXDOC + block_rows
    keys_padded = jnp.concatenate([jnp.zeros((MAXDOC, HD), key_rows.dtype), key_rows], axis=0)
    values_padded = jnp.concatenate([jnp.zeros((MAXDOC, HD), value_rows.dtype), value_rows], axis=0)
    segment_padded = jnp.concatenate([jnp.full((MAXDOC,), -1, jnp.int32), segment.astype(jnp.int32)], axis=0)

    def one_block(running, index):
        key_total, value_total = running
        start = (index * block_rows).astype(jnp.int32)
        query_block = lax.dynamic_slice_in_dim(queries, start, block_rows, 0).astype(jnp.float32).reshape(block_rows, HEADS, HD)
        grad_block = lax.dynamic_slice_in_dim(out_grad, start, block_rows, 0).astype(jnp.float32).reshape(block_rows, HEADS, HD)
        query_seg = lax.dynamic_slice_in_dim(segment.astype(jnp.int32), start, block_rows, 0)
        key_window = lax.dynamic_slice_in_dim(keys_padded, start, window, 0).astype(jnp.float32)
        value_window = lax.dynamic_slice_in_dim(values_padded, start, window, 0).astype(jnp.float32)
        key_seg = lax.dynamic_slice_in_dim(segment_padded, start, window, 0)
        query_pos = start + jnp.arange(block_rows, dtype=jnp.int32)
        key_pos = start - MAXDOC + jnp.arange(window, dtype=jnp.int32)
        visible = (key_seg[None, :] == query_seg[:, None]) & (key_pos[None, :] <= query_pos[:, None])
        visible = visible[:, None, :]
        scores = jnp.einsum("thd,kd->thk", query_block, key_window) * score_scale
        row_max = jnp.max(jnp.where(visible, scores, -1e30), axis=-1)
        row_sum = jnp.sum(jnp.where(visible, jnp.exp(scores - row_max[..., None]), 0.0), axis=-1)
        log_total = row_max + jnp.log(row_sum)
        prob = jnp.where(visible, jnp.exp(scores - log_total[..., None]), 0.0)
        weight = prob.astype(jnp.bfloat16)
        attended = jnp.einsum("thk,kd->thd", weight.astype(jnp.float32), value_window).astype(jnp.bfloat16)
        row_dot = jnp.sum(grad_block * attended.astype(jnp.float32), axis=-1)
        dprob = jnp.einsum("thd,kd->thk", grad_block, value_window)
        dscore = (score_scale * prob * (dprob - row_dot[..., None])).astype(jnp.bfloat16)
        query_grad = jnp.einsum("thk,kd->thd", dscore.astype(jnp.float32), key_window).astype(jnp.bfloat16)
        key_part = jnp.einsum("thk,thd->kd", dscore.astype(jnp.float32), query_block)
        value_part = jnp.einsum("thk,thd->kd", weight.astype(jnp.float32), grad_block)
        key_total = lax.dynamic_update_slice_in_dim(key_total, lax.dynamic_slice_in_dim(key_total, start, window, 0) + key_part, start, 0)
        value_total = lax.dynamic_update_slice_in_dim(value_total, lax.dynamic_slice_in_dim(value_total, start, window, 0) + value_part, start, 0)
        return (key_total, value_total), (attended.reshape(block_rows, HEADS * HD), query_grad.reshape(block_rows, HEADS * HD))

    start_totals = (jnp.zeros((MAXDOC + TOKENS, HD), jnp.float32), jnp.zeros((MAXDOC + TOKENS, HD), jnp.float32))
    totals, outputs = lax.scan(one_block, start_totals, jnp.arange(block_count, dtype=jnp.int32))
    attended = outputs[0].reshape(TOKENS, HEADS * HD)
    query_grad = outputs[1].reshape(TOKENS, HEADS * HD)
    return attended, query_grad, totals[0][MAXDOC:], totals[1][MAXDOC:]
```

```python
import functools
import math

import jax
import jax.numpy as jnp
from jax import lax
from jax.experimental import pallas as pl
from jax.experimental.pallas import tpu as pltpu
from jax.sharding import PartitionSpec as P

MAXDOC = 1536
AXES = ("seq", "grp")
MESH = pl.DeviceIdType.MESH
F32 = jnp.float32
BF16 = jnp.bfloat16
HIDDEN = -1e30


def dot_nt(a, b):
    return lax.dot_general(a, b, (((1,), (1,)), ((), ())), preferred_element_type=F32)


def dot_nn(a, b):
    return lax.dot_general(a, b, (((1,), (0,)), ((), ())), preferred_element_type=F32)


def kernel(
    groups, total, span,
    q_ref, k_ref, v_ref, g_ref, seg_ref,
    o_ref, dq_ref, dk_ref, dv_ref,
    keys, values, segs, qs, gs, gt, bias, scores, probs, weight,
    row_max, row_sum, row_inv, row_dot,
    gk_out, gv_out, gk_in, gv_in,
    k_send, k_recv, s_send, s_recv, v_send, v_recv, gk_send, gk_recv, gv_send, gv_recv,
):
    tokens, width = k_ref.shape
    heads = q_ref.shape[1] // width
    scale = width ** -0.5
    exponent = scale * math.log2(math.e)
    me = lax.axis_index("seq") * groups + lax.axis_index("grp")

    def device_at(distance):
        where = lax.rem(me + distance + total, total)
        return (lax.div(where, groups), lax.rem(where, groups))

    def rows(d):
        return pl.ds(pl.multiple_of(d * tokens, tokens), tokens)

    def key_copy(d):
        return pltpu.make_async_remote_copy(
            src_ref=k_ref, dst_ref=keys.at[rows(d)], send_sem=k_send.at[d], recv_sem=k_recv.at[d],
            device_id=device_at(d), device_id_type=MESH)

    def seg_copy(d):
        return pltpu.make_async_remote_copy(
            src_ref=seg_ref, dst_ref=segs.at[d], send_sem=s_send.at[d], recv_sem=s_recv.at[d],
            device_id=device_at(d), device_id_type=MESH)

    def value_copy(d):
        return pltpu.make_async_remote_copy(
            src_ref=v_ref, dst_ref=values.at[rows(d)], send_sem=v_send.at[d], recv_sem=v_recv.at[d],
            device_id=device_at(d), device_id_type=MESH)

    def key_grad_copy(d):
        return pltpu.make_async_remote_copy(
            src_ref=gk_out.at[d], dst_ref=gk_in.at[d], send_sem=gk_send.at[d],
            recv_sem=gk_recv.at[d], device_id=device_at(-d), device_id_type=MESH)

    def value_grad_copy(d):
        return pltpu.make_async_remote_copy(
            src_ref=gv_out.at[d], dst_ref=gv_in.at[d], send_sem=gv_send.at[d],
            recv_sem=gv_recv.at[d], device_id=device_at(-d), device_id_type=MESH)

    barrier = pltpu.get_barrier_semaphore()
    for d in range(1, span + 1):
        for way in (d, -d):
            pl.semaphore_signal(barrier, inc=1, device_id=device_at(way), device_id_type=MESH)

    keys[pl.ds(0, tokens), :] = k_ref[...]
    values[pl.ds(0, tokens), :] = v_ref[...]
    segs[0] = seg_ref[...]
    for h in range(heads):
        stacked = pl.ds(h * tokens, tokens)
        head = pl.ds(h * width, width)
        qs[stacked, :] = q_ref[:, head]
        gs[stacked, :] = g_ref[:, head]
        gt[:, stacked] = g_ref[:, head].T
    row_max[...] = jnp.full(row_max.shape, HIDDEN, F32)
    row_sum[...] = jnp.zeros(row_sum.shape, F32)

    pl.semaphore_wait(barrier, 2 * span)
    for d in range(1, span + 1):
        key_copy(d).start()
        seg_copy(d).start()
    for d in range(1, span + 1):
        value_copy(d).start()

    def score_pass(d, carry):
        @pl.when(d > 0)
        def _():
            key_copy(d).wait_recv()
            seg_copy(d).wait_recv()

        key_block = keys[rows(d), :]
        seg_column = jnp.broadcast_to(segs[d][0:1, :], (128, tokens)).T
        seg_key = jnp.concatenate([seg_column] * (tokens // 128), axis=1)
        key_at = lax.broadcasted_iota(jnp.int32, (tokens, tokens), 0) - d * tokens
        query_at = lax.broadcasted_iota(jnp.int32, (tokens, tokens), 1)
        first = jnp.where(me >= d, -d * tokens, tokens)
        visible = (seg_key == seg_ref[0:1, :]) & (key_at <= query_at) & (key_at >= first)
        bias[...] = jnp.where(visible, 0.0, HIDDEN)
        for h in range(heads):
            cols = pl.ds(h * tokens, tokens)
            score = dot_nt(key_block, qs[cols, :]) + bias[...]
            scores[rows(d), cols] = score
            top = jnp.max(score.reshape(tokens // 8, 8, tokens), axis=0)
            row_max[:, cols] = jnp.maximum(row_max[:, cols], top)
        return carry

    lax.fori_loop(0, span + 1, score_pass, 0)
    row_max[...] = jnp.broadcast_to(jnp.max(row_max[...], axis=0, keepdims=True), row_max.shape)

    def exp_pass(d, carry):
        for h in range(heads):
            cols = pl.ds(h * tokens, tokens)
            part = jnp.exp2((scores[rows(d), cols] - row_max[0:1, cols]) * exponent)
            row_sum[:, cols] += jnp.sum(part.reshape(tokens // 8, 8, tokens), axis=0)
            probs[rows(d), cols] = part.astype(BF16)
        return carry

    lax.fori_loop(0, span + 1, exp_pass, 0)
    for d in range(1, span + 1):
        value_copy(d).wait_recv()
    values_t = values[...].T
    for h in range(heads):
        cols = pl.ds(h * tokens, tokens)
        inverse = 1.0 / jnp.sum(row_sum[:, cols], axis=0, keepdims=True)
        attended = (dot_nn(values_t, probs[:, cols]) * inverse).astype(BF16)
        dot = jnp.sum(attended.astype(F32) * gt[:, cols].astype(F32), axis=0, keepdims=True)
        row_inv[:, cols] = jnp.broadcast_to(inverse, (8, tokens))
        row_dot[:, cols] = jnp.broadcast_to(dot, (8, tokens))
        o_ref[:, pl.ds(h * width, width)] = attended.T

    def grad_pass(step, carry):
        d = span - step
        value_block = values[rows(d), :]
        for h in range(heads):
            cols = pl.ds(h * tokens, tokens)
            dprob = dot_nt(value_block, gs[cols, :])
            prob = probs[rows(d), cols].astype(F32) * row_inv[0:1, cols]
            weight[:, cols] = prob.astype(BF16)
            probs[rows(d), cols] = (prob * (dprob - row_dot[0:1, cols])).astype(BF16)
        key_part = dot_nn(probs[rows(d), :], qs[...]) * scale
        value_part = dot_nn(weight[...], gs[...])

        @pl.when(d > 0)
        def _():
            gk_out[d] = key_part.astype(BF16)
            gv_out[d] = value_part.astype(BF16)
            key_grad_copy(d).start()
            value_grad_copy(d).start()

        @pl.when(d == 0)
        def _():
            dk_ref[...] = key_part
            dv_ref[...] = value_part

        return carry

    lax.fori_loop(0, span + 1, grad_pass, 0)
    keys_t = keys[...].T
    for h in range(heads):
        cols = pl.ds(h * tokens, tokens)
        grad = (dot_nn(keys_t, probs[:, cols]) * scale).astype(BF16)
        dq_ref[:, pl.ds(h * width, width)] = grad.T
    for d in range(span, 0, -1):
        key_grad_copy(d).wait_recv()
        value_grad_copy(d).wait_recv()
        dk_ref[...] += gk_in[d].astype(F32)
        dv_ref[...] += gv_in[d].astype(F32)
    for d in range(1, span + 1):
        key_copy(d).wait_send()
        seg_copy(d).wait_send()
        value_copy(d).wait_send()
        key_grad_copy(d).wait_send()
        value_grad_copy(d).wait_send()


def on_device(queries, key_rows, value_rows, out_grad, segment):
    tokens, width = key_rows.shape
    heads = queries.shape[1] // width
    groups = lax.axis_size("grp")
    total = groups * lax.axis_size("seq")
    span = -(-MAXDOC // tokens)
    blocks = span + 1
    stacked = heads * tokens
    seg_rows = jnp.broadcast_to(segment.astype(F32)[None, :], (8, tokens))
    vmem = pl.BlockSpec(memory_space=pltpu.VMEM)
    sems = pltpu.SemaphoreType.DMA((blocks,))
    return pl.pallas_call(
        functools.partial(kernel, groups, total, span),
        out_shape=(
            jax.ShapeDtypeStruct(queries.shape, BF16),
            jax.ShapeDtypeStruct(queries.shape, BF16),
            jax.ShapeDtypeStruct(key_rows.shape, F32),
            jax.ShapeDtypeStruct(key_rows.shape, F32),
        ),
        in_specs=[vmem] * 5,
        out_specs=(vmem,) * 4,
        scratch_shapes=[
            pltpu.VMEM((blocks * tokens, width), BF16),
            pltpu.VMEM((blocks * tokens, width), BF16),
            pltpu.VMEM((blocks, 8, tokens), F32),
            pltpu.VMEM((stacked, width), BF16),
            pltpu.VMEM((stacked, width), BF16),
            pltpu.VMEM((width, stacked), BF16),
            pltpu.VMEM((tokens, tokens), F32),
            pltpu.VMEM((blocks * tokens, stacked), F32),
            pltpu.VMEM((blocks * tokens, stacked), BF16),
            pltpu.VMEM((tokens, stacked), BF16),
            pltpu.VMEM((8, stacked), F32),
            pltpu.VMEM((8, stacked), F32),
            pltpu.VMEM((8, stacked), F32),
            pltpu.VMEM((8, stacked), F32),
            pltpu.VMEM((blocks, tokens, width), BF16),
            pltpu.VMEM((blocks, tokens, width), BF16),
            pltpu.VMEM((blocks, tokens, width), BF16),
            pltpu.VMEM((blocks, tokens, width), BF16),
        ]
        + [sems] * 10,
        compiler_params=pltpu.CompilerParams(
            collective_id=0, has_side_effects=True, vmem_limit_bytes=60 * 1024 * 1024
        ),
    )(queries, key_rows, value_rows, out_grad, seg_rows)


def solution(mesh):
    in_specs = (P(AXES, None), P(AXES, None), P(AXES, None), P(AXES, None), P(AXES))
    out_specs = (P(AXES, None),) * 4
    return jax.shard_map(
        on_device, mesh=mesh, in_specs=in_specs, out_specs=out_specs, check_vma=False
    )
```
